256 devices in a mesh: dp: 4 (over y), expert: 32 (over x, z), etp: 2 (over core).
Axes of the slice: x: 4, y: 4, z: 8, core: 2. Of those that a mesh axis runs over, the one named last changes fastest.
Arguments:
- tokens: bfloat16 [8192, 4096], P(('dp', 'expert'), 'etp'), may hold values from -6 to 6
- expert_ids: int32 [8192, 8], P(('dp', 'expert')), may hold values from 0 to 63, all different within a row; in each aligned block of 64 rows (0 to 63, 64 to 127, ...) at most 12 rows name the same one
- combine: float32 [8192, 8], P(('dp', 'expert')), may hold values from 0.05 to 1
- gate_weight: bfloat16 [64, 4096, 1536], P('expert', 'dp', 'etp'), may hold values from -0.09375 to 0.09375
- up_weight: bfloat16 [64, 4096, 1536], P('expert', 'dp', 'etp'), may hold values from -0.09375 to 0.09375
- down_weight: bfloat16 [64, 1536, 4096], P('expert', 'etp', 'dp'), may hold values from -0.15625 to 0.15625
Outputs:
- mixed: bfloat16 [8192, 4096], P(('dp', 'expert'), 'etp')
The draws below stay inside these ranges and needn't reach their ends.
Inputs may be any that keep to these rules, and one draw needn't show every extreme that they name: `expert_ids`: each row names 8 different experts. In the rows of one device (aligned blocks of 64 rows) no expert is named by more than 12 rows, a bound that some block reaches.
All inputs are finite; a program needn't handle non-finite values.
Results may differ from the reference program's by a relative error of at most 0.008.
Values may be sent and summed in bfloat16 or wider, within the bound.
No kernel may reach another device: no remote copies, remote signals or barrier semaphores. Data moves between devices by JAX's collectives and lax.ppermute only.
A program may use at most 192 MiB of HBM per device.

```python
import math
import jax
import jax.numpy as jnp
import numpy as np
from jax import lax

D = 4096
FF = 1536
TOP = 8
TOK_DEV = 64
EXPERTS = 64
TOKENS = 8192
CAP = 12
N_DP = 4
N_EXPERT = 32
N_ETP = 2


def block_scale(rng, shape, pieces, smallest, high):
    level = 1.0
    for axis_at, blocks in pieces:
        steps = jax.random.uniform(jax.random.fold_in(jax.random.fold_in(rng, 6), axis_at), (blocks,), jnp.float32, smallest / len(pieces), high / len(pieces))
        level = level * jnp.repeat(jnp.exp(steps), shape[axis_at] // blocks).reshape((-1,) + (1,) * (len(shape) - 1 - axis_at))
    return level


def routed_block(own_key, own, number, rows, count, top, limit, lean):
    order = jax.random.permutation(own_key, count)
    heavy_load, common = shares(count, rows * top, limit, lean, True), shares(count, rows * top, limit, lean, False)
    places = jnp.arange(count)

    def named(tallies, turn):
        used = int((tallies > 0).sum())
        fixed = max(1, used // 4)
        shifted = fixed + (places - fixed + turn * (used - fixed)) % max(1, count - fixed)
        return jnp.zeros((count,), jnp.int32).at[order[jnp.where(places < fixed, places, shifted)]].set(jnp.asarray(tallies, jnp.int32))

    tallies = jnp.where(number % 4 == 0, named(heavy_load, number // 4), named(common, number - number // 4 - 1))
    mixed = jax.random.permutation(jax.random.fold_in(own, 3), count)
    source_of, sink = mixed[0:count // 2 * 2:2], mixed[1:count // 2 * 2:2]
    slack = jnp.minimum(tallies[source_of] - 1, limit - tallies[sink]) // 2
    slack = jnp.where((source_of == order[0]) | (sink == order[0]) | (tallies[sink] == 0), 0, jnp.maximum(slack, 0))
    shifted = jax.random.randint(jax.random.fold_in(own, 4), (count // 2,), 0, 1 << 20) % (slack + 1)
    tallies = tallies.at[source_of].add(-shifted).at[sink].add(shifted)
    members = jnp.searchsorted(jnp.cumsum(tallies), jnp.arange(rows * top), side="right").astype(jnp.int32)
    table = members.reshape(top, rows).T
    table = table[jax.random.permutation(jax.random.fold_in(own, 1), rows)]
    turn = jax.random.randint(jax.random.fold_in(own, 2), (rows, 1), 0, top)
    return jnp.take_along_axis(table, (jnp.arange(top)[None, :] + turn) % top, axis=1)


def shares(number_of, total, limit, skew, full):
    weights = [(1 << 20) // math.isqrt(rank ** skew) + 1 for rank in range(1, number_of + 1)]
    largest = limit if full else min(limit, max(-(-total // number_of), total * weights[0] // sum(weights)))
    least = 1 if total - largest >= number_of - 1 else 0
    given, spare = [largest] + [least] * (number_of - 1), total - largest - least * (number_of - 1)
    while spare > 0:
        candidates = [i for i in range(1, number_of) if given[i] < largest] or [i for i in range(1, number_of) if given[i] < limit]
        mass, remaining = sum([weights[i] for i in candidates]), spare
        for i in candidates:
            more = min(limit - given[i], max(1, remaining * weights[i] // mass), spare)
            given[i] = given[i] + more
            spare = spare - more
    return np.array(given)


def noise(key, shape, scale, limit, cuts=(), kind=jnp.bfloat16):
    entries = scale * jax.random.normal(key, shape, jnp.float32)
    if cuts:
        entries = entries * block_scale(key, shape, cuts, -0.22, 0.18)
    return jnp.clip(entries, -limit, limit).astype(kind)


def setup_inputs(seed: int = 0) -> dict:
    arg_keys = jax.random.split(jax.random.key(seed), 7)
    tokens = noise(arg_keys[0], (TOKENS, D), 1.0, 6.0, ((0, 128), (1, 2)))
    expert_ids_keys = jax.random.split(jax.random.fold_in(arg_keys[1], 1), TOKENS // TOK_DEV)
    expert_ids_turns = jax.random.permutation(jax.random.fold_in(arg_keys[1], 3), TOKENS // TOK_DEV)
    expert_ids = jax.vmap(lambda own, number: routed_block(jax.random.fold_in(arg_keys[1], 2), own, number, TOK_DEV, EXPERTS, TOP, CAP, 2))(expert_ids_keys, expert_ids_turns).reshape((TOKENS, TOP))
    combine = jnp.clip(jnp.exp(math.log(1.0) - 2.9957323 * jax.random.uniform(arg_keys[2], (TOKENS, TOP), jnp.float32) ** block_scale(arg_keys[2], (TOKENS, TOP), ((0, 128),), -0.2, 0.2)), 0.05, 1.0)
    gate_weight = noise(arg_keys[3], (EXPERTS, D, FF), D ** -0.5, 0.09375, ((0, 32), (1, 4), (2, 2)))
    up_weight = noise(arg_keys[4], (EXPERTS, D, FF), D ** -0.5, 0.09375, ((0, 32), (1, 4), (2, 2)))
    down_weight = noise(arg_keys[5], (EXPERTS, FF, D), FF ** -0.5, 0.15625, ((0, 32), (1, 2), (2, 4)))
    return dict(tokens=tokens, expert_ids=expert_ids, combine=combine, gate_weight=gate_weight, up_weight=up_weight, down_weight=down_weight)


def reference(tokens, expert_ids, combine, gate_weight, up_weight, down_weight):
    tok_rows = tokens.shape[0]
    rows_max = N_DP * N_EXPERT * CAP
    share = FF // N_ETP

    def one_expert(running, expert):
        selected = expert_ids == expert
        chosen = jnp.any(selected, axis=1)
        weight = jnp.sum(jnp.where(selected, combine, 0.0), axis=1)
        ordering = jnp.cumsum(chosen.astype(jnp.int32)) - 1
        placement = jnp.where(chosen, ordering, rows_max).astype(jnp.int32)
        row_index = jnp.zeros((rows_max + 1,), jnp.int32).at[placement].set(jnp.arange(tok_rows, dtype=jnp.int32))
        row_block = tokens[row_index[:rows_max]]
        gate_sum = jnp.dot(row_block, gate_weight[expert], preferred_element_type=jnp.float32)
        up_sum = jnp.dot(row_block, up_weight[expert], preferred_element_type=jnp.float32)
        hidden = (jax.nn.silu(gate_sum) * up_sum).astype(jnp.bfloat16)
        summed = jnp.zeros((rows_max, tokens.shape[1]), jnp.float32)
        for shard in range(N_ETP):
            partial_value = jnp.dot(hidden[:, shard * share:(shard + 1) * share], down_weight[expert][shard * share:(shard + 1) * share], preferred_element_type=jnp.float32).astype(jnp.bfloat16)
            partial_value = lax.optimization_barrier(partial_value)
            summed = summed + partial_value.astype(jnp.float32)
        expert_out = summed.astype(jnp.bfloat16)
        gathered = expert_out[jnp.clip(ordering, 0, rows_max - 1)].astype(jnp.float32)
        running = running + jnp.where(chosen[:, None], weight[:, None] * gathered, 0.0)
        return running, None

    start_sum = jnp.zeros(tokens.shape, jnp.float32)
    total, unused = lax.scan(one_expert, start_sum, jnp.arange(gate_weight.shape[0], dtype=jnp.int32))
    return total.astype(jnp.bfloat16)
```

```python
import jax
import jax.numpy as jnp
from jax import lax
from jax.experimental import pallas as pl
from jax.experimental.pallas import tpu as pltpu
from jax.sharding import PartitionSpec as P


BF = jnp.bfloat16
F32 = jnp.float32
META = 128
PLAN = (('pack', 0), ('share', 0), ('gate_up', 0), ('pack', 1), ('pass', 0), ('act', 0), ('share', 1), ('gate_up', 1), ('relay', 0), ('pass', 1), ('down', 0), ('act', 1), ('relay', 1), ('down', 1), ('mix', 0), ('mix', 1))


def whole(shape):
    return pl.BlockSpec(shape, lambda i, p: (0,) * len(shape))


def call(body, place, arrays, specs, outs, flops):
    return pl.pallas_call(
        body,
        grid_spec=pltpu.PrefetchScalarGridSpec(
            num_scalar_prefetch=1,
            grid=(1,),
            in_specs=[spec or whole(array.shape) for array, spec in zip(arrays, specs)],
            out_specs=[whole(shape) for shape in outs],
        ),
        out_shape=[jax.ShapeDtypeStruct(shape, BF) for shape in outs],
        cost_estimate=pl.CostEstimate(flops=flops, bytes_accessed=5_000_000, transcendentals=0),
    )(place, *arrays)


def times(rows, at, weight, out, out_at, base):
    product = jnp.dot(rows[at, :], weight[...], preferred_element_type=F32)
    out[out_at, pl.ds(base, weight.shape[1])] = product.astype(BF)


def gate_up(mine, other, gate_weight, up_weight, place, expert):
    count, width = mine.shape
    hidden = gate_weight.shape[2]
    piece = count // 4

    def body(place_ref, a_ref, b_ref, g_ref, u_ref, ahead, behind, nxt_a, prv_b, own_a, own_b):
        first, second = pl.ds(0, piece), pl.ds(piece, piece)
        jobs = (
            (a_ref, 2, ahead, first), (b_ref, 1, ahead, second), (b_ref, 2, behind, first), (a_ref, 3, behind, second),
            (a_ref, 1, nxt_a, first), (b_ref, 3, prv_b, first), (a_ref, 0, own_a, first), (b_ref, 0, own_b, first),
        )
        for rows, step, out, at in jobs:
            start = pl.multiple_of(lax.rem(place_ref[0] + step, 4) * piece, piece)
            times(rows, pl.ds(start, piece), g_ref, out, at, 0)
            times(rows, pl.ds(start, piece), u_ref, out, at, hidden)

    spec = pl.BlockSpec((None, width, hidden), lambda i, p: (expert, 0, 0))
    return call(
        body, place, (mine, other, gate_weight, up_weight), (None, None, spec, spec),
        [(2 * piece, 2 * hidden)] * 2 + [(piece, 2 * hidden)] * 4, 8 * count * width * hidden,
    )


def passed_on(nxt_a, prv_b, ahead, behind, place):
    piece, both = nxt_a.shape

    def body(place_ref, nxt_ref, prv_ref, ahead_ref, behind_ref, send_a, send_b):
        send_a[...] = (nxt_ref[...].astype(F32) + ahead_ref[...].astype(F32)).astype(BF)
        send_b[...] = (prv_ref[...].astype(F32) + behind_ref[...].astype(F32)).astype(BF)

    half = pl.BlockSpec((piece, both), lambda i, p: (0, 0))
    return call(body, place, (nxt_a, prv_b, ahead, behind), (None, None, half, half), [(piece, both)] * 2, 10**8)


def activated(own_a, own_b, got_a, got_b, ahead, behind, place):
    piece, both = own_a.shape
    hidden = both // 2

    def body(place_ref, own_a, own_b, got_a, got_b, ahead, behind, out):
        for at, own, got, rest in ((0, own_a, got_a, behind), (piece, own_b, got_b, ahead)):
            total = own[...].astype(F32) + got[...].astype(F32) + rest[...].astype(F32)
            out[pl.ds(at, piece), :] = (jax.nn.silu(total[:, :hidden]) * total[:, hidden:]).astype(BF)

    half = pl.BlockSpec((piece, both), lambda i, p: (1, 0))
    return call(
        body, place, (own_a, own_b, got_a, got_b, ahead, behind), (None,) * 4 + (half, half),
        [(2 * piece, hidden)], 10**8,
    )[0]


def down(own, nxt, prv, opp_a, opp_b, down_weight, place, expert):
    piece, hidden = opp_a.shape
    width = down_weight.shape[2]

    def body(place_ref, own, nxt, prv, opp_a, opp_b, w_ref, out_a, out_b):
        first, second = pl.ds(0, piece), pl.ds(piece, piece)
        jobs = (
            (own, second, 0, out_b), (nxt, second, 1, out_b), (prv, second, 3, out_b), (opp_b, first, 2, out_b),
            (own, first, 0, out_a), (nxt, first, 1, out_a), (prv, first, 3, out_a), (opp_a, first, 2, out_a),
        )
        for rows, at, step, out in jobs:
            start = pl.multiple_of(lax.rem(place_ref[0] + step, 4) * piece, piece)
            times(rows, at, w_ref, out, pl.ds(start, piece), 0)

    spec = pl.BlockSpec((None, hidden, width), lambda i, p: (expert, 0, 0))
    return call(
        body, place, (own, nxt, prv, opp_a, opp_b, down_weight), (None,) * 5 + (spec,),
        [(4 * piece, width)] * 2, 16 * piece * width * hidden,
    )


def shards(tokens, expert_ids, combine, gate_weight, up_weight, down_weight):
    tok_rows, top_count = expert_ids.shape
    held = gate_weight.shape[0]
    groups = lax.axis_size("expert")
    ring = lax.axis_size("dp")
    experts = held * groups
    capacity = min(tok_rows, 3 * tok_rows * top_count // (2 * experts))
    width = gate_weight.shape[1]
    dp = lax.axis_index("dp")
    place = dp.astype(jnp.int32).reshape(1)

    def forward(array):
        return lax.ppermute(array, "dp", [(i, (i + 1) % ring) for i in range(ring)])

    def backward(array):
        return lax.ppermute(array, "dp", [(i, (i - 1) % ring) for i in range(ring)])

    def partner(array):
        return lax.ppermute(array, "etp", [(0, 1), (1, 0)])

    def sends(turn):
        return [
            (2 * d0 + s, 2 * (2 * s + (d0 + turn) % 2) + d0 // 2) for d0 in range(ring) for s in range(2)
        ]

    high = combine.astype(BF)
    low = (combine - high.astype(F32)).astype(BF)
    meta = jnp.concatenate(
        [expert_ids.astype(BF), high, low, jnp.zeros((tok_rows, META - 3 * top_count), BF)], axis=1
    )

    def payload(turn):
        features = lax.dynamic_slice_in_dim(tokens, ((dp + turn) % 2) * width, width, axis=1)
        return jnp.concatenate([features, meta], axis=1)

    came = [lax.ppermute(payload(turn), ("dp", "etp"), sends(turn)) for turn in range(2)]
    even = dp % 2 == 0
    blocks = jnp.stack([jnp.where(even, came[0], came[1]), jnp.where(even, came[1], came[0])])
    features = blocks[:, :, :width].reshape(2 * tok_rows, width)
    ids = blocks[:, :, width : width + top_count].astype(F32)
    weight_high = blocks[:, :, width + top_count : width + 2 * top_count]
    weight_low = blocks[:, :, width + 2 * top_count : width + 3 * top_count]

    named = ids[:, :, :, None] == jnp.arange(experts, dtype=F32)[None, None, None, :]
    chosen = jnp.any(named, axis=2)
    lower = (jnp.arange(tok_rows)[:, None] >= jnp.arange(tok_rows)[None, :]).astype(BF)
    rank = jnp.einsum("ut,bte->bue", lower, chosen.astype(BF), preferred_element_type=F32)
    rank = jnp.where(chosen, rank, 0.0)

    def spread(values):
        picked = jnp.where(named, values.astype(F32)[:, :, :, None], 0.0)
        return jnp.sum(picked, axis=2).astype(BF)

    high_map, low_map = spread(weight_high), spread(weight_low)
    slots = jnp.arange(1, capacity + 1, dtype=F32)
    same = jnp.eye(2, dtype=jnp.bool_)

    def by_expert(values, expert):
        return values.reshape(2, tok_rows, groups, held)[:, :, :, expert]

    slots_all = 2 * capacity
    chunks = ((0, 0, slots_all), (1, 0, slots_all))

    def hits(chunk):
        expert, low_row, high_row = chunk
        mine = by_expert(rank, expert)
        hit = (mine[:, :, :, None, None] == slots) & same[:, None, None, :, None]
        return hit.reshape(2 * tok_rows, groups, slots_all)[:, :, low_row:high_row]

    state = [{} for _ in chunks]
    total = jnp.zeros((2 * tok_rows, width), F32)
    last = ()

    def after(*values):
        nonlocal last
        if not last:
            return values
        values, last = lax.optimization_barrier((values, last))
        return values

    for stage, at in PLAN:
        chunk, s = chunks[at], state[at]
        if stage == "pack":
            picker = hits(chunk).astype(BF).reshape(2 * tok_rows, -1)
            packed = lax.dot_general(picker, features, (((0,), (0,)), ((), ())), preferred_element_type=F32)
            (packed,) = after(packed.astype(BF).reshape(groups, -1, width))
            s["came"] = lax.all_to_all(packed, "expert", 0, 0, tiled=True)
            last = (packed,)
        elif stage == "share":
            (came,) = after(s["came"])
            s["mine"] = came.reshape(-1, width)
            s["other"] = partner(s["mine"])
            last = (came,)
        elif stage == "gate_up":
            mine, other = after(s["mine"], s["other"])
            ahead, behind, *s["kept"] = gate_up(mine, other, gate_weight, up_weight, place, chunk[0])
            s["ahead"], s["behind"] = forward(ahead), backward(behind)
            last = (ahead, behind)
        elif stage == "pass":
            ahead, behind = s["ahead"], s["behind"] = after(s["ahead"], s["behind"])
            send_a, send_b = passed_on(*s["kept"][:2], ahead, behind, place)
            s["got_a"], s["got_b"] = forward(send_a), backward(send_b)
            last = (send_a, send_b)
        elif stage == "act":
            got_a, got_b = after(s["got_a"], s["got_b"])
            s["own"] = activated(*s["kept"][2:], got_a, got_b, s["ahead"], s["behind"], place)
            s["prv"], s["nxt"] = forward(s["own"]), backward(s["own"])
            last = (s["own"],)
        elif stage == "relay":
            prv, nxt = s["prv"], s["nxt"] = after(s["prv"], s["nxt"])
            half = prv.shape[0] // 2
            send_a, send_b = prv[:half], nxt[half:]
            s["opp_a"], s["opp_b"] = forward(send_a), backward(send_b)
            last = (send_a, send_b)
        elif stage == "down":
            opp_a, opp_b = after(s["opp_a"], s["opp_b"])
            part_a, part_b = down(s["own"], s["nxt"], s["prv"], opp_a, opp_b, down_weight, place, chunk[0])
            out = (part_a.astype(F32) + partner(part_b).astype(F32)).astype(BF)
            s["back"] = lax.all_to_all(out.reshape(groups, -1, width), "expert", 0, 0, tiled=True)
            last = (out,)
        else:
            (back,) = after(s["back"])
            hit = hits(chunk)
            for weights in (high_map, low_map):
                placed = jnp.where(hit, by_expert(weights, chunk[0]).reshape(2 * tok_rows, groups, 1), 0).astype(BF)
                total = total + jnp.dot(
                    placed.reshape(2 * tok_rows, -1), back.reshape(-1, width), preferred_element_type=F32
                )
            last = (total,)
    mixed = total.astype(BF).reshape(2, tok_rows, width)

    result = []
    for turn in range(2):
        block = jnp.where((dp + turn) % 2 == 0, mixed[0], mixed[1])
        result.append(lax.ppermute(block, ("dp", "etp"), [(b, a) for a, b in sends(turn)]))
    return jnp.concatenate(
        [jnp.where(even, result[0], result[1]), jnp.where(even, result[1], result[0])], axis=1
    )


def solution(mesh):
    placed = (
        P(("dp", "expert"), "etp"),
        P(("dp", "expert"), None),
        P(("dp", "expert"), None),
        P("expert", "dp", "etp"),
        P("expert", "dp", "etp"),
        P("expert", "etp", "dp"),
    )

    return jax.shard_map(shards, mesh=mesh, in_specs=placed, out_specs=P(("dp", "expert"), "etp"), check_vma=False)
```

```python
import jax
import jax.numpy as jnp
from jax import lax
from jax.experimental import pallas as pl
from jax.experimental.pallas import tpu as pltpu
from jax.sharding import PartitionSpec as P


BF = jnp.bfloat16
F32 = jnp.float32
META = 128
PLAN = (('pack', 0), ('share', 0), ('first', 0), ('second', 0), ('pack', 1), ('pass', 0), ('act', 0), ('share', 1), ('relay', 0), ('gate_up', 1), ('down', 0), ('pass', 1), ('return', 0), ('act', 1), ('relay', 1), ('down', 1), ('return', 1), ('mix', 0), ('mix', 1))


def whole(shape):
    return pl.BlockSpec(shape, lambda i, p: (0,) * len(shape))


def call(body, place, arrays, specs, outs, flops, scratch=()):
    return pl.pallas_call(
        body,
        grid_spec=pltpu.PrefetchScalarGridSpec(
            num_scalar_prefetch=1,
            grid=(1,),
            in_specs=[spec or whole(array.shape) for array, spec in zip(arrays, specs)],
            out_specs=[whole(shape) for shape in outs],
            scratch_shapes=[pltpu.VMEM(shape, BF) for shape in scratch],
        ),
        out_shape=[jax.ShapeDtypeStruct(shape, BF) for shape in outs],
        cost_estimate=pl.CostEstimate(flops=flops, bytes_accessed=5_000_000, transcendentals=0),
    )(place, *arrays)


def gate_up(mine, other, gate_weight, up_weight, place, expert):
    count, width = mine.shape
    hidden = gate_weight.shape[2]
    piece = count // 4

    def body(place_ref, a_ref, b_ref, g_ref, u_ref, *refs):
        outs, held, sums = refs[:5], refs[5], refs[6]
        jobs = ((a_ref, 2), (b_ref, 2), (b_ref, 1), (a_ref, 3), (a_ref, 1), (b_ref, 3), (a_ref, 0), (b_ref, 0))
        for number, (rows, step) in enumerate(jobs):
            start = pl.multiple_of(lax.rem(place_ref[0] + step, 4) * piece, piece)
            held[number * piece : (number + 1) * piece, :] = rows[pl.ds(start, piece), :]

        def multiply(number, carry):
            x = held[pl.ds(pl.multiple_of(number * piece, piece), piece), :]
            for half, weight in enumerate((g_ref, u_ref)):
                product = jnp.dot(x, weight[...], preferred_element_type=F32)
                sums[:, half * hidden : (half + 1) * hidden] = product.astype(BF)
            for at, out in enumerate(outs[:4]):

                @pl.when(number == at)
                def _():
                    out[...] = sums[...]

            @pl.when(number >= 4)
            def _():
                outs[4][pl.ds(pl.multiple_of((number - 4) * piece, piece), piece), :] = sums[...]

            return carry

        lax.fori_loop(0, 8, multiply, 0)

    spec = pl.BlockSpec((None, width, hidden), lambda i, p: (expert, 0, 0))
    return call(
        body, place, (mine, other, gate_weight, up_weight), (None, None, spec, spec),
        [(piece, 2 * hidden)] * 4 + [(4 * piece, 2 * hidden)], 8 * count * width * hidden, [(8 * piece, width), (piece, 2 * hidden)],
    )


def gate_up_half(rows, gate_weight, up_weight, place, expert, steps):
    count, width = rows.shape
    hidden = gate_weight.shape[2]
    piece = count // 4

    def body(place_ref, x_ref, g_ref, u_ref, one, two, kept, held, sums):
        for number, step in enumerate(steps):
            start = pl.multiple_of(lax.rem(place_ref[0] + step, 4) * piece, piece)
            held[number * piece : (number + 1) * piece, :] = x_ref[pl.ds(start, piece), :]

        def multiply(number, carry):
            x = held[pl.ds(pl.multiple_of(number * piece, piece), piece), :]
            for half, weight in enumerate((g_ref, u_ref)):
                product = jnp.dot(x, weight[...], preferred_element_type=F32)
                sums[:, half * hidden : (half + 1) * hidden] = product.astype(BF)
            for at, out in enumerate((one, two)):

                @pl.when(number == at)
                def _():
                    out[...] = sums[...]

            @pl.when(number >= 2)
            def _():
                kept[pl.ds(pl.multiple_of((number - 2) * piece, piece), piece), :] = sums[...]

            return carry

        lax.fori_loop(0, 4, multiply, 0)

    spec = pl.BlockSpec((None, width, hidden), lambda i, p: (expert, 0, 0))
    return call(
        body, place, (rows, gate_weight, up_weight), (None, spec, spec),
        [(piece, 2 * hidden)] * 2 + [(2 * piece, 2 * hidden)], 4 * count * width * hidden,
        [(4 * piece, width), (piece, 2 * hidden)],
    )


def block(piece, width, number):
    return pl.BlockSpec((piece, width), lambda i, p: (number, 0))


def passed_on(nxt_a, prv_b, got_a, got_b, place):
    piece, both = got_a.shape

    def body(place_ref, nxt_ref, prv_ref, got_a_ref, got_b_ref, send_a, send_b):
        send_a[...] = (nxt_ref[...].astype(F32) + got_a_ref[...].astype(F32)).astype(BF)
        send_b[...] = (prv_ref[...].astype(F32) + got_b_ref[...].astype(F32)).astype(BF)

    specs = [block(piece, both, number) for number in (nxt_a[1], prv_b[1], 0, 0)]
    return call(body, place, (nxt_a[0], prv_b[0], got_a, got_b), specs, [(piece, both)] * 2, 10**8)


def activated(own_a, own_b, got_a, got_b, rest_a, rest_b, place):
    piece, both = got_a.shape
    hidden = both // 2

    def body(place_ref, own_a, own_b, got_a, got_b, rest_a, rest_b, out):
        for at, own, got, rest in ((0, own_a, got_a, rest_a), (piece, own_b, got_b, rest_b)):
            total = own[...].astype(F32) + got[...].astype(F32) + rest[...].astype(F32)
            out[pl.ds(at, piece), :] = (jax.nn.silu(total[:, :hidden]) * total[:, hidden:]).astype(BF)

    specs = [block(piece, both, number) for number in (own_a[1], own_b[1], 0, 0, 0, 0)]
    return call(body, place, (own_a[0], own_b[0], got_a, got_b, rest_a, rest_b), specs, [(2 * piece, hidden)], 10**8)[0]


def down(own, nxt, prv, opp_a, opp_b, down_weight, place, expert):
    piece, hidden = opp_a.shape
    width = down_weight.shape[2]

    def body(place_ref, own, nxt, prv, opp_a, opp_b, w_ref, out_a, out_b, held):
        for half, opp in enumerate((opp_a, opp_b)):
            for step, rows in ((0, own), (1, nxt), (3, prv), (2, opp)):
                at = half * piece if step != 2 else 0
                start = pl.multiple_of((half * 4 + lax.rem(place_ref[0] + step, 4)) * piece, piece)
                held[pl.ds(start, piece), :] = rows[at : at + piece, :]
        for half, out in enumerate((out_a, out_b)):

            def multiply(number, carry):
                start = pl.multiple_of(number * piece, piece)
                x = held[pl.ds(half * 4 * piece + start, piece), :]
                out[pl.ds(start, piece), :] = jnp.dot(x, w_ref[...], preferred_element_type=F32).astype(BF)
                return carry

            lax.fori_loop(0, 4, multiply, 0)

    spec = pl.BlockSpec((None, hidden, width), lambda i, p: (expert, 0, 0))
    return call(
        body, place, (own, nxt, prv, opp_a, opp_b, down_weight), (None,) * 5 + (spec,),
        [(4 * piece, width)] * 2, 16 * piece * width * hidden, [(8 * piece, hidden)],
    )


def shards(tokens, expert_ids, combine, gate_weight, up_weight, down_weight):
    tok_rows, top_count = expert_ids.shape
    held = gate_weight.shape[0]
    groups = lax.axis_size("expert")
    ring = lax.axis_size("dp")
    experts = held * groups
    capacity = min(tok_rows, 3 * tok_rows * top_count // (2 * experts))
    width = gate_weight.shape[1]
    dp = lax.axis_index("dp")
    place = dp.astype(jnp.int32).reshape(1)

    def forward(array):
        return lax.ppermute(array, "dp", [(i, (i + 1) % ring) for i in range(ring)])

    def backward(array):
        return lax.ppermute(array, "dp", [(i, (i - 1) % ring) for i in range(ring)])

    def partner(array):
        return lax.ppermute(array, "etp", [(0, 1), (1, 0)])

    def sends(turn):
        return [
            (2 * d0 + s, 2 * (2 * s + (d0 + turn) % 2) + d0 // 2) for d0 in range(ring) for s in range(2)
        ]

    high = combine.astype(BF)
    low = (combine - high.astype(F32)).astype(BF)
    meta = jnp.concatenate(
        [expert_ids.astype(BF), high, low, jnp.zeros((tok_rows, META - 3 * top_count), BF)], axis=1
    )

    def payload(turn):
        features = lax.dynamic_slice_in_dim(tokens, ((dp + turn) % 2) * width, width, axis=1)
        return jnp.concatenate([features, meta], axis=1)

    came = [lax.ppermute(payload(turn), ("dp", "etp"), sends(turn)) for turn in range(2)]
    even = dp % 2 == 0
    blocks = jnp.stack([jnp.where(even, came[0], came[1]), jnp.where(even, came[1], came[0])])
    features = blocks[:, :, :width].reshape(2 * tok_rows, width)
    ids = blocks[:, :, width : width + top_count].astype(F32)
    weight_high = blocks[:, :, width + top_count : width + 2 * top_count]
    weight_low = blocks[:, :, width + 2 * top_count : width + 3 * top_count]

    named = ids[:, :, :, None] == jnp.arange(experts, dtype=F32)[None, None, None, :]
    chosen = jnp.any(named, axis=2)
    lower = (jnp.arange(tok_rows)[:, None] >= jnp.arange(tok_rows)[None, :]).astype(BF)
    rank = jnp.einsum("ut,bte->bue", lower, chosen.astype(BF), preferred_element_type=F32)
    rank = jnp.where(chosen, rank, 0.0)

    def spread(values):
        picked = jnp.where(named, values.astype(F32)[:, :, :, None], 0.0)
        return jnp.sum(picked, axis=2).astype(BF)

    high_map, low_map = spread(weight_high), spread(weight_low)
    slots = jnp.arange(1, capacity + 1, dtype=F32)
    same = jnp.eye(2, dtype=jnp.bool_)

    def by_expert(values, expert):
        return values.reshape(2, tok_rows, groups, held)[:, :, :, expert]

    slots_all = 2 * capacity
    chunks = ((0, 0, slots_all), (1, 0, slots_all))

    def hits(chunk):
        expert, low_row, high_row = chunk
        mine = by_expert(rank, expert)
        hit = (mine[:, :, :, None, None] == slots) & same[:, None, None, :, None]
        return hit.reshape(2 * tok_rows, groups, slots_all)[:, :, low_row:high_row]

    state = [{} for _ in chunks]
    total = jnp.zeros((2 * tok_rows, width), F32)
    last = ()

    def after(*values):
        nonlocal last
        if not last:
            return values
        values, last = lax.optimization_barrier((values, last))
        return values

    for stage, at in PLAN:
        chunk, s = chunks[at], state[at]
        if stage == "pack":
            picker = hits(chunk).astype(BF).reshape(2 * tok_rows, -1)
            packed = lax.dot_general(picker, features, (((0,), (0,)), ((), ())), preferred_element_type=F32)
            (packed,) = after(packed.astype(BF).reshape(groups, -1, width))
            s["came"] = lax.all_to_all(packed, "expert", 0, 0, tiled=True)
            last = (packed,)
        elif stage == "share":
            (came,) = after(s["came"])
            s["mine"] = came.reshape(-1, width)
            s["other"] = partner(s["mine"])
            last = (came,)
        elif stage == "gate_up":
            mine, other = after(s["mine"], s["other"])
            opp_a, opp_b, nxt_b, prv_a, kept = gate_up(
                mine, other, gate_weight, up_weight, place, chunk[0]
            )
            s["kept"] = [(kept, number) for number in range(4)]
            s["ahead"], s["behind"] = forward(opp_a), backward(opp_b)
            s["nxt_b"], s["prv_a"] = forward(nxt_b), backward(prv_a)
            last = (opp_a,)
        elif stage == "first":
            (mine,) = after(s["mine"])
            opp_a, s["send"], kept_a = gate_up_half(mine, gate_weight, up_weight, place, chunk[0], (2, 3, 1, 0))
            s["kept"] = [(kept_a, 0), None, (kept_a, 1), None]
            s["ahead"] = forward(opp_a)
            last = (opp_a,)
        elif stage == "second":
            (other,) = after(s["other"])
            opp_b, nxt_b, kept_b = gate_up_half(other, gate_weight, up_weight, place, chunk[0], (2, 1, 3, 0))
            s["kept"][1], s["kept"][3] = (kept_b, 0), (kept_b, 1)
            s["behind"] = backward(opp_b)
            s["nxt_b"], s["prv_a"] = forward(nxt_b), backward(s["send"])
            last = (opp_b,)
        elif stage == "pass":
            ahead, behind = s["ahead"], s["behind"] = after(s["ahead"], s["behind"])
            send_a, send_b = passed_on(*s["kept"][:2], ahead, behind, place)
            s["got_a"], s["got_b"] = forward(send_a), backward(send_b)
            last = (send_a, send_b)
        elif stage == "act":
            got_a, got_b, prv_a, nxt_b = after(s["got_a"], s["got_b"], s["prv_a"], s["nxt_b"])
            s["own"] = activated(*s["kept"][2:], got_a, got_b, prv_a, nxt_b, place)
            s["prv"], s["nxt"] = forward(s["own"]), backward(s["own"])
            last = (s["own"],)
        elif stage == "relay":
            prv, nxt = s["prv"], s["nxt"] = after(s["prv"], s["nxt"])
            half = prv.shape[0] // 2
            send_a, send_b = prv[:half], nxt[half:]
            s["opp_a"], s["opp_b"] = forward(send_a), backward(send_b)
            last = (send_a, send_b)
        elif stage == "down":
            opp_a, opp_b = after(s["opp_a"], s["opp_b"])
            part_a, part_b = down(s["own"], s["nxt"], s["prv"], opp_a, opp_b, down_weight, place, chunk[0])
            s["part"], s["got"] = part_a, partner(part_b)
            last = (part_a,)
        elif stage == "return":
            (got,) = after(s["got"])
            out = (s["part"].astype(F32) + got.astype(F32)).astype(BF)
            s["back"] = lax.all_to_all(out.reshape(groups, -1, width), "expert", 0, 0, tiled=True)
            last = (out,)
        else:
            (back,) = after(s["back"])
            hit = hits(chunk)
            for weights in (high_map, low_map):
                placed = jnp.where(hit, by_expert(weights, chunk[0]).reshape(2 * tok_rows, groups, 1), 0).astype(BF)
                total = total + jnp.dot(
                    placed.reshape(2 * tok_rows, -1), back.reshape(-1, width), preferred_element_type=F32
                )
            last = (total,)
    mixed = total.astype(BF).reshape(2, tok_rows, width)

    result = []
    for turn in range(2):
        block = jnp.where((dp + turn) % 2 == 0, mixed[0], mixed[1])
        result.append(lax.ppermute(block, ("dp", "etp"), [(b, a) for a, b in sends(turn)]))
    return jnp.concatenate(
        [jnp.where(even, result[0], result[1]), jnp.where(even, result[1], result[0])], axis=1
    )


def solution(mesh):
    placed = (
        P(("dp", "expert"), "etp"),
        P(("dp", "expert"), None),
        P(("dp", "expert"), None),
        P("expert", "dp", "etp"),
        P("expert", "dp", "etp"),
        P("expert", "etp", "dp"),
    )

    return jax.shard_map(shards, mesh=mesh, in_specs=placed, out_specs=P(("dp", "expert"), "etp"), check_vma=False)
```

```python
import jax
import jax.numpy as jnp
from jax import lax
from jax.experimental import pallas as pl
from jax.experimental.pallas import tpu as pltpu
from jax.sharding import PartitionSpec as P


BF = jnp.bfloat16
F32 = jnp.float32
META = 128
PLAN = (('pack', 0), ('share', 0), ('first', 0), ('second', 0), ('pack', 1), ('pass', 0), ('act', 0), ('share', 1), ('relay', 0), ('gate_up', 1), ('down', 0), ('pass', 1), ('return', 0), ('act', 1), ('relay', 1), ('down', 1), ('return', 1), ('mix', 0), ('mix', 1))


def whole(shape):
    return pl.BlockSpec(shape, lambda i, p: (0,) * len(shape))


def call(body, place, arrays, specs, outs, flops, scratch=()):
    return pl.pallas_call(
        body,
        grid_spec=pltpu.PrefetchScalarGridSpec(
            num_scalar_prefetch=1,
            grid=(1,),
            in_specs=[spec or whole(array.shape) for array, spec in zip(arrays, specs)],
            out_specs=[whole(shape) for shape in outs],
            scratch_shapes=[pltpu.VMEM(shape, BF) for shape in scratch],
        ),
        out_shape=[jax.ShapeDtypeStruct(shape, BF) for shape in outs],
        cost_estimate=pl.CostEstimate(flops=flops, bytes_accessed=5_000_000, transcendentals=0),
    )(place, *arrays)


def gate_up(mine, other, gate_weight, up_weight, place, expert):
    count, width = mine.shape
    hidden = gate_weight.shape[2]
    piece = count // 4

    def body(place_ref, a_ref, b_ref, g_ref, u_ref, *refs):
        outs, held, sums = refs[:5], refs[5], refs[6]
        jobs = ((a_ref, 2), (b_ref, 2), (b_ref, 1), (a_ref, 3), (a_ref, 1), (b_ref, 3), (a_ref, 0), (b_ref, 0))
        for number, (rows, step) in enumerate(jobs):
            start = pl.multiple_of(lax.rem(place_ref[0] + step, 4) * piece, piece)
            held[number * piece : (number + 1) * piece, :] = rows[pl.ds(start, piece), :]

        def multiply(number, carry):
            x = held[pl.ds(pl.multiple_of(number * piece, piece), piece), :]
            for half, weight in enumerate((g_ref, u_ref)):
                product = jnp.dot(x, weight[...], preferred_element_type=F32)
                sums[:, half * hidden : (half + 1) * hidden] = product.astype(BF)
            for at, out in enumerate(outs[:4]):

                @pl.when(number == at)
                def _():
                    out[...] = sums[...]

            @pl.when(number >= 4)
            def _():
                outs[4][pl.ds(pl.multiple_of((number - 4) * piece, piece), piece), :] = sums[...]

            return carry

        lax.fori_loop(0, 8, multiply, 0)

    spec = pl.BlockSpec((None, width, hidden), lambda i, p: (expert, 0, 0))
    return call(
        body, place, (mine, other, gate_weight, up_weight), (None, None, spec, spec),
        [(piece, 2 * hidden)] * 4 + [(4 * piece, 2 * hidden)], 8 * count * width * hidden, [(8 * piece, width), (piece, 2 * hidden)],
    )


def gate_up_half(rows, gate_weight, up_weight, place, expert, steps):
    count, width = rows.shape
    hidden = gate_weight.shape[2]
    piece = count // 4

    def body(place_ref, x_ref, g_ref, u_ref, one, two, kept, held, sums):
        for number, step in enumerate(steps):
            start = pl.multiple_of(lax.rem(place_ref[0] + step, 4) * piece, piece)
            held[number * piece : (number + 1) * piece, :] = x_ref[pl.ds(start, piece), :]

        def multiply(number, carry):
            x = held[pl.ds(pl.multiple_of(number * piece, piece), piece), :]
            for half, weight in enumerate((g_ref, u_ref)):
                product = jnp.dot(x, weight[...], preferred_element_type=F32)
                sums[:, half * hidden : (half + 1) * hidden] = product.astype(BF)
            for at, out in enumerate((one, two)):

                @pl.when(number == at)
                def _():
                    out[...] = sums[...]

            @pl.when(number >= 2)
            def _():
                kept[pl.ds(pl.multiple_of((number - 2) * piece, piece), piece), :] = sums[...]

            return carry

        lax.fori_loop(0, 4, multiply, 0)

    spec = pl.BlockSpec((None, width, hidden), lambda i, p: (expert, 0, 0))
    return call(
        body, place, (rows, gate_weight, up_weight), (None, spec, spec),
        [(piece, 2 * hidden)] * 2 + [(2 * piece, 2 * hidden)], 4 * count * width * hidden,
        [(4 * piece, width), (piece, 2 * hidden)],
    )


def block(piece, width, number):
    return pl.BlockSpec((piece, width), lambda i, p: (number, 0))


def passed_on(nxt_a, prv_b, got_a, got_b, place):
    piece, both = got_a.shape

    def body(place_ref, nxt_ref, prv_ref, got_a_ref, got_b_ref, send_a, send_b):
        send_a[...] = (nxt_ref[...].astype(F32) + got_a_ref[...].astype(F32)).astype(BF)
        send_b[...] = (prv_ref[...].astype(F32) + got_b_ref[...].astype(F32)).astype(BF)

    specs = [block(piece, both, number) for number in (nxt_a[1], prv_b[1], 0, 0)]
    return call(body, place, (nxt_a[0], prv_b[0], got_a, got_b), specs, [(piece, both)] * 2, 10**8)


def activated(own_a, own_b, got_a, got_b, rest_a, rest_b, place):
    piece, both = got_a.shape
    hidden = both // 2

    def body(place_ref, own_a, own_b, got_a, got_b, rest_a, rest_b, out):
        for at, own, got, rest in ((0, own_a, got_a, rest_a), (piece, own_b, got_b, rest_b)):
            total = own[...].astype(F32) + got[...].astype(F32) + rest[...].astype(F32)
            out[pl.ds(at, piece), :] = (jax.nn.silu(total[:, :hidden]) * total[:, hidden:]).astype(BF)

    specs = [block(piece, both, number) for number in (own_a[1], own_b[1], 0, 0, 0, 0)]
    return call(body, place, (own_a[0], own_b[0], got_a, got_b, rest_a, rest_b), specs, [(2 * piece, hidden)], 10**8)[0]


def down(own, nxt, prv, opp, half, down_weight, place, expert):
    piece, hidden = opp.shape
    width = down_weight.shape[2]

    def body(place_ref, own, nxt, prv, opp, w_ref, out, held):
        for step, rows in ((0, own), (1, nxt), (3, prv), (2, opp)):
            start = pl.multiple_of(lax.rem(place_ref[0] + step, 4) * piece, piece)
            held[pl.ds(start, piece), :] = rows[...]

        def multiply(number, carry):
            start = pl.multiple_of(number * piece, piece)
            x = held[pl.ds(start, piece), :]
            out[pl.ds(start, piece), :] = jnp.dot(x, w_ref[...], preferred_element_type=F32).astype(BF)
            return carry

        lax.fori_loop(0, 4, multiply, 0)

    spec = pl.BlockSpec((None, hidden, width), lambda i, p: (expert, 0, 0))
    rows_spec = block(piece, hidden, half)
    return call(
        body, place, (own, nxt, prv, opp, down_weight), (rows_spec, rows_spec, rows_spec, None, spec),
        [(4 * piece, width)], 8 * piece * width * hidden, [(4 * piece, hidden)],
    )[0]


def shards(tokens, expert_ids, combine, gate_weight, up_weight, down_weight):
    tok_rows, top_count = expert_ids.shape
    held = gate_weight.shape[0]
    groups = lax.axis_size("expert")
    ring = lax.axis_size("dp")
    experts = held * groups
    capacity = min(tok_rows, 3 * tok_rows * top_count // (2 * experts))
    width = gate_weight.shape[1]
    dp = lax.axis_index("dp")
    place = dp.astype(jnp.int32).reshape(1)

    def forward(array):
        return lax.ppermute(array, "dp", [(i, (i + 1) % ring) for i in range(ring)])

    def backward(array):
        return lax.ppermute(array, "dp", [(i, (i - 1) % ring) for i in range(ring)])

    def partner(array):
        return lax.ppermute(array, "etp", [(0, 1), (1, 0)])

    def sends(turn):
        return [
            (2 * d0 + s, 2 * (2 * s + (d0 + turn) % 2) + d0 // 2) for d0 in range(ring) for s in range(2)
        ]

    high = combine.astype(BF)
    low = (combine - high.astype(F32)).astype(BF)
    meta = jnp.concatenate(
        [expert_ids.astype(BF), high, low, jnp.zeros((tok_rows, META - 3 * top_count), BF)], axis=1
    )

    def payload(turn):
        features = lax.dynamic_slice_in_dim(tokens, ((dp + turn) % 2) * width, width, axis=1)
        return jnp.concatenate([features, meta], axis=1)

    came = [lax.ppermute(payload(turn), ("dp", "etp"), sends(turn)) for turn in range(2)]
    even = dp % 2 == 0
    blocks = jnp.stack([jnp.where(even, came[0], came[1]), jnp.where(even, came[1], came[0])])
    features = blocks[:, :, :width].reshape(2 * tok_rows, width)
    ids = blocks[:, :, width : width + top_count].astype(F32)
    weight_high = blocks[:, :, width + top_count : width + 2 * top_count]
    weight_low = blocks[:, :, width + 2 * top_count : width + 3 * top_count]

    named = ids[:, :, :, None] == jnp.arange(experts, dtype=F32)[None, None, None, :]
    chosen = jnp.any(named, axis=2)
    lower = (jnp.arange(tok_rows)[:, None] >= jnp.arange(tok_rows)[None, :]).astype(BF)
    rank = jnp.einsum("ut,bte->bue", lower, chosen.astype(BF), preferred_element_type=F32)
    rank = jnp.where(chosen, rank, 0.0)

    def spread(values):
        picked = jnp.where(named, values.astype(F32)[:, :, :, None], 0.0)
        return jnp.sum(picked, axis=2).astype(BF)

    high_map, low_map = spread(weight_high), spread(weight_low)
    slots = jnp.arange(1, capacity + 1, dtype=F32)
    same = jnp.eye(2, dtype=jnp.bool_)

    def by_expert(values, expert):
        return values.reshape(2, tok_rows, groups, held)[:, :, :, expert]

    slots_all = 2 * capacity
    chunks = ((0, 0, slots_all), (1, 0, slots_all))

    def hits(chunk):
        expert, low_row, high_row = chunk
        mine = by_expert(rank, expert)
        hit = (mine[:, :, :, None, None] == slots) & same[:, None, None, :, None]
        return hit.reshape(2 * tok_rows, groups, slots_all)[:, :, low_row:high_row]

    state = [{} for _ in chunks]
    total = jnp.zeros((2 * tok_rows, width), F32)
    last = ()

    def after(*values):
        nonlocal last
        if not last:
            return values
        values, last = lax.optimization_barrier((values, last))
        return values

    for stage, at in PLAN:
        chunk, s = chunks[at], state[at]
        if stage == "pack":
            picker = hits(chunk).astype(BF).reshape(2 * tok_rows, -1)
            packed = lax.dot_general(picker, features, (((0,), (0,)), ((), ())), preferred_element_type=F32)
            (packed,) = after(packed.astype(BF).reshape(groups, -1, width))
            s["came"] = lax.all_to_all(packed, "expert", 0, 0, tiled=True)
            last = (packed,)
        elif stage == "share":
            (came,) = after(s["came"])
            s["mine"] = came.reshape(-1, width)
            s["other"] = partner(s["mine"])
            last = (came,)
        elif stage == "gate_up":
            mine, other = after(s["mine"], s["other"])
            opp_a, opp_b, nxt_b, prv_a, kept = gate_up(
                mine, other, gate_weight, up_weight, place, chunk[0]
            )
            s["kept"] = [(kept, number) for number in range(4)]
            s["ahead"], s["behind"] = forward(opp_a), backward(opp_b)
            s["nxt_b"], s["prv_a"] = forward(nxt_b), backward(prv_a)
            last = (opp_a,)
        elif stage == "first":
            (mine,) = after(s["mine"])
            opp_a, s["send"], kept_a = gate_up_half(mine, gate_weight, up_weight, place, chunk[0], (2, 3, 1, 0))
            s["kept"] = [(kept_a, 0), None, (kept_a, 1), None]
            s["ahead"] = forward(opp_a)
            last = (opp_a,)
        elif stage == "second":
            (other,) = after(s["other"])
            opp_b, nxt_b, kept_b = gate_up_half(other, gate_weight, up_weight, place, chunk[0], (2, 1, 3, 0))
            s["kept"][1], s["kept"][3] = (kept_b, 0), (kept_b, 1)
            s["behind"] = backward(opp_b)
            s["nxt_b"], s["prv_a"] = forward(nxt_b), backward(s["send"])
            last = (opp_b,)
        elif stage == "pass":
            ahead, behind = s["ahead"], s["behind"] = after(s["ahead"], s["behind"])
            send_a, send_b = passed_on(*s["kept"][:2], ahead, behind, place)
            s["got_a"], s["got_b"] = forward(send_a), backward(send_b)
            last = (send_a, send_b)
        elif stage == "act":
            got_a, got_b, prv_a, nxt_b = after(s["got_a"], s["got_b"], s["prv_a"], s["nxt_b"])
            s["own"] = activated(*s["kept"][2:], got_a, got_b, prv_a, nxt_b, place)
            s["prv"], s["nxt"] = forward(s["own"]), backward(s["own"])
            last = (s["own"],)
        elif stage == "relay":
            prv, nxt = s["prv"], s["nxt"] = after(s["prv"], s["nxt"])
            half = prv.shape[0] // 2
            send_a, send_b = prv[:half], nxt[half:]
            s["opp_a"], s["opp_b"] = forward(send_a), backward(send_b)
            last = (send_a, send_b)
        elif stage == "down":
            opp_a, opp_b = after(s["opp_a"], s["opp_b"])
            rows = (s["own"], s["nxt"], s["prv"])
            part_b = down(*rows, opp_b, 1, down_weight, place, chunk[0])
            s["got"] = partner(part_b)
            opp_a, part_b = lax.optimization_barrier((opp_a, part_b))
            s["part"] = down(*rows, opp_a, 0, down_weight, place, chunk[0])
            last = (s["part"],)
        elif stage == "return":
            (got,) = after(s["got"])
            out = (s["part"].astype(F32) + got.astype(F32)).astype(BF)
            s["back"] = lax.all_to_all(out.reshape(groups, -1, width), "expert", 0, 0, tiled=True)
            last = (out,)
        else:
            (back,) = after(s["back"])
            hit = hits(chunk)
            for weights in (high_map, low_map):
                placed = jnp.where(hit, by_expert(weights, chunk[0]).reshape(2 * tok_rows, groups, 1), 0).astype(BF)
                total = total + jnp.dot(
                    placed.reshape(2 * tok_rows, -1), back.reshape(-1, width), preferred_element_type=F32
                )
            last = (total,)
    mixed = total.astype(BF).reshape(2, tok_rows, width)

    result = []
    for turn in range(2):
        block = jnp.where((dp + turn) % 2 == 0, mixed[0], mixed[1])
        result.append(lax.ppermute(block, ("dp", "etp"), [(b, a) for a, b in sends(turn)]))
    return jnp.concatenate(
        [jnp.where(even, result[0], result[1]), jnp.where(even, result[1], result[0])], axis=1
    )


def solution(mesh):
    placed = (
        P(("dp", "expert"), "etp"),
        P(("dp", "expert"), None),
        P(("dp", "expert"), None),
        P("expert", "dp", "etp"),
        P("expert", "dp", "etp"),
        P("expert", "etp", "dp"),
    )

    return jax.shard_map(shards, mesh=mesh, in_specs=placed, out_specs=P(("dp", "expert"), "etp"), check_vma=False)
```
